16 devices in a mesh: req: 4 (over z, y), dap: 4 (over x, core).
Axes of the slice: x: 2, y: 2, z: 2, core: 2. Of those that a mesh axis runs over, the one named last changes fastest.
Arguments:
- msa_act: bfloat16 [256, 256, 256], P(('req', 'dap')), parts along dimension 0
- pair_act: bfloat16 [1024, 256, 128], P(('req', 'dap')), parts along dimension 0
- msa_mask: int32 [256, 256], P(('req', 'dap')), parts along dimension 0
- pair_mask: int32 [1024, 256], P(('req', 'dap')), parts along dimension 0
- row_qkvg: bfloat16 [2, 256, 1024], replicated
- row_bias: bfloat16 [2, 128, 8], replicated
- row_out: bfloat16 [2, 256, 256], replicated
- col_qkvg: bfloat16 [2, 256, 1024], replicated
- col_out: bfloat16 [2, 256, 256], replicated
- mtr_in: bfloat16 [2, 256, 1024], replicated
- mtr_out: bfloat16 [2, 1024, 256], replicated
- opm_proj: bfloat16 [2, 256, 64], replicated
- opm_out: bfloat16 [2, 1024, 128], replicated
- tmo_proj: bfloat16 [2, 128, 640], replicated
- tmo_out: bfloat16 [2, 128, 128], replicated
- tmi_proj: bfloat16 [2, 128, 640], replicated
- tmi_out: bfloat16 [2, 128, 128], replicated
- tas_qkvg: bfloat16 [2, 128, 512], replicated
- tas_bias: bfloat16 [2, 128, 4], replicated
- tas_out: bfloat16 [2, 128, 128], replicated
- tae_qkvg: bfloat16 [2, 128, 512], replicated
- tae_bias: bfloat16 [2, 128, 4], replicated
- tae_out: bfloat16 [2, 128, 128], replicated
- ptr_in: bfloat16 [2, 128, 512], replicated
- ptr_out: bfloat16 [2, 512, 128], replicated
Outputs:
- output 1: bfloat16 [256, 256, 256], P(('req', 'dap')), parts along dimension 0
- output 2: bfloat16 [1024, 256, 128], P(('req', 'dap')), parts along dimension 0
There are 4 independent parts. The reference program is written for one: setup_inputs(seed, part) draws one part's arguments, and reference() takes and returns one part's arrays. A program takes and returns all parts, laid end to end along the dimension named above; an argument that names none is the same for every part.
All inputs are finite; a program needn't handle non-finite values.
Results may differ from the reference program's by a relative error of at most 0.02.
Values are sent between devices in bfloat16 or wider.
A program may use at most 1 GiB of HBM per device.

```python
import jax
import jax.numpy as jnp
from jax import lax

SEQ = 64
RES = 256
MSA_DIM = 256
PAIR_DIM = 128
MSA_HEADS = 8
MSA_HEAD_DIM = 32
PAIR_HEADS = 4
PAIR_HEAD_DIM = 32
OPM_DIM = 32
TRI_DIM = 128
LAYERS = 2

WEIGHT_NAMES = ('row_qkvg', 'row_bias', 'row_out', 'col_qkvg', 'col_out', 'mtr_in', 'mtr_out', 'opm_proj', 'opm_out', 'tmo_proj', 'tmo_out', 'tmi_proj', 'tmi_out', 'tas_qkvg', 'tas_bias', 'tas_out', 'tae_qkvg', 'tae_bias', 'tae_out', 'ptr_in', 'ptr_out')


def weight_fans():
    msa_width = MSA_HEADS * MSA_HEAD_DIM
    pair_width = PAIR_HEADS * PAIR_HEAD_DIM
    return ((MSA_DIM, 4 * msa_width), (PAIR_DIM, MSA_HEADS), (msa_width, MSA_DIM),
            (MSA_DIM, 4 * msa_width), (msa_width, MSA_DIM),
            (MSA_DIM, 4 * MSA_DIM), (4 * MSA_DIM, MSA_DIM),
            (MSA_DIM, 2 * OPM_DIM), (OPM_DIM * OPM_DIM, PAIR_DIM),
            (PAIR_DIM, 4 * TRI_DIM + PAIR_DIM), (TRI_DIM, PAIR_DIM),
            (PAIR_DIM, 4 * TRI_DIM + PAIR_DIM), (TRI_DIM, PAIR_DIM),
            (PAIR_DIM, 4 * pair_width), (PAIR_DIM, PAIR_HEADS), (pair_width, PAIR_DIM),
            (PAIR_DIM, 4 * pair_width), (PAIR_DIM, PAIR_HEADS), (pair_width, PAIR_DIM),
            (PAIR_DIM, 4 * PAIR_DIM), (4 * PAIR_DIM, PAIR_DIM))


def draw_masks(mask_key):
    key_list = jax.random.split(mask_key, 4)
    pad_len = jax.random.randint(key_list[0], (), 1, RES // 16 + 1)
    res_ids = jnp.arange(RES)
    seq_ids = jnp.arange(SEQ)[:, None]
    is_valid = res_ids < RES - pad_len
    shallow = jax.random.randint(key_list[1], (RES,), 0, 4) == 0
    depths = jnp.where(shallow, jax.random.randint(key_list[2], (RES,), 1, SEQ // 4 + 1), SEQ)
    kept_mask = (jax.random.randint(key_list[3], (SEQ, RES), 0, 8) != 0) | (seq_ids == 0)
    msa_mask = ((seq_ids < depths[None, :]) & kept_mask & is_valid[None, :]).astype(jnp.int32)
    pair_mask = (is_valid[:, None] & is_valid[None, :]).astype(jnp.int32)
    return msa_mask, pair_mask


def setup_inputs(seed: int = 0, part: int = 0) -> dict:
    part_key = jax.random.fold_in(jax.random.key(seed), part)
    key_list = jax.random.split(part_key, 3)
    shared = jax.random.normal(key_list[0], (1, RES, MSA_DIM), jnp.float32)
    spread = jax.random.normal(key_list[1], (SEQ, RES, MSA_DIM), jnp.float32)
    msa_act = (shared + spread).astype(jnp.bfloat16)
    pair_act = jax.random.normal(key_list[2], (RES, RES, PAIR_DIM), jnp.float32).astype(jnp.bfloat16)
    msa_mask, pair_mask = draw_masks(jax.random.fold_in(part_key, 5))
    inputs = {'msa_act': msa_act, 'pair_act': pair_act, 'msa_mask': msa_mask, 'pair_mask': pair_mask}
    weight_key = jax.random.key(seed + 1)
    for w_index, fan_pair in enumerate(weight_fans()):
        sample = jax.random.normal(jax.random.fold_in(weight_key, w_index), (LAYERS,) + fan_pair, jnp.float32)
        inputs[WEIGHT_NAMES[w_index]] = (sample * fan_pair[0] ** -0.5).astype(jnp.bfloat16)
    return inputs


def layer_norm(x):
    values = x.astype(jnp.float32)
    centered = values - jnp.mean(values, axis=-1, keepdims=True)
    variance = jnp.mean(centered * centered, axis=-1, keepdims=True)
    return (centered * lax.rsqrt(variance + 1e-5)).astype(jnp.bfloat16)


def linear(x, weight):
    flat_x = x.reshape(-1, x.shape[-1])
    result = jnp.dot(flat_x, weight, preferred_element_type=jnp.float32)
    return result.reshape(x.shape[:-1] + (weight.shape[-1],))


def residual(x, update):
    return (x.astype(jnp.float32) + update).astype(jnp.bfloat16)


def attend_row(x_row, bias_hij, mask_row, w_qkvg, w_out, num_heads):
    length = x_row.shape[0]
    head_width = w_out.shape[0]
    head_dim = head_width // num_heads
    projected = jnp.dot(x_row, w_qkvg, preferred_element_type=jnp.float32).astype(jnp.bfloat16).astype(jnp.float32)
    queries = projected[:, :head_width].reshape(length, num_heads, head_dim)
    keyset = projected[:, head_width:2 * head_width].reshape(length, num_heads, head_dim)
    valset = projected[:, 2 * head_width:3 * head_width].reshape(length, num_heads, head_dim)
    gate_act = jax.nn.sigmoid(projected[:, 3 * head_width:])
    logits = jnp.einsum('ihd,jhd->hij', queries, keyset) * head_dim ** -0.5 + bias_hij.astype(jnp.float32)
    logits = jnp.where(mask_row[None, None, :] > 0, logits, -1e9)
    attn_prob = jax.nn.softmax(logits, axis=-1).astype(jnp.bfloat16).astype(jnp.float32)
    attended = jnp.einsum('hij,jhd->ihd', attn_prob, valset).reshape(length, head_width)
    gated = (attended * gate_act).astype(jnp.bfloat16)
    return jnp.dot(gated, w_out, preferred_element_type=jnp.float32)


def row_attention(msa_act, pair_act, msa_mask, w_qkvg, w_bias, w_out):
    pair_bias = jnp.transpose(linear(layer_norm(pair_act), w_bias).astype(jnp.bfloat16), (2, 0, 1))
    msa_norm = layer_norm(msa_act)
    return lax.map(lambda item: attend_row(item[0], pair_bias, item[1], w_qkvg, w_out, w_bias.shape[1]), (msa_norm, msa_mask))


def column_attention(msa_act, msa_mask, w_qkvg, w_out, num_heads):
    msa_norm = jnp.swapaxes(layer_norm(msa_act), 0, 1)
    zero_bias = jnp.zeros((1, 1, 1), jnp.float32)
    update = lax.map(lambda item: attend_row(item[0], zero_bias, item[1], w_qkvg, w_out, num_heads), (msa_norm, msa_mask.T))
    return jnp.swapaxes(update, 0, 1)


def transition(x, w_in, w_out):
    hidden = jnp.maximum(linear(layer_norm(x), w_in), 0.0).astype(jnp.bfloat16)
    return linear(hidden, w_out)


def outer_product_mean(msa_act, msa_mask, w_proj, w_out):
    opm_dim = w_proj.shape[1] // 2
    projected = linear(layer_norm(msa_act), w_proj).astype(jnp.bfloat16)
    mask_bf = msa_mask.astype(jnp.bfloat16)[:, :, None]
    left_act = (projected[..., :opm_dim] * mask_bf).astype(jnp.float32)
    right_act = (projected[..., opm_dim:] * mask_bf).astype(jnp.float32)
    mask_f = msa_mask.astype(jnp.float32)
    overlap = jnp.dot(mask_f.T, mask_f)

    def outer_row(left_row):
        outer_prod = jnp.einsum('sc,sje->jce', left_row, right_act).astype(jnp.bfloat16)
        return linear(outer_prod.reshape(outer_prod.shape[0], opm_dim * opm_dim), w_out)

    update = lax.map(outer_row, jnp.swapaxes(left_act, 0, 1))
    return update / (1e-3 + overlap)[:, :, None]


def tri_mul(pair_act, pair_mask, w_proj, w_out, form):
    tri_dim = (w_proj.shape[1] - pair_act.shape[-1]) // 4
    projected = linear(layer_norm(pair_act), w_proj)
    mask_f = pair_mask.astype(jnp.float32)[:, :, None]
    left_act = (mask_f * jax.nn.sigmoid(projected[..., 2 * tri_dim:3 * tri_dim]) * projected[..., :tri_dim]).astype(jnp.bfloat16)
    right_act = (mask_f * jax.nn.sigmoid(projected[..., 3 * tri_dim:4 * tri_dim]) * projected[..., tri_dim:2 * tri_dim]).astype(jnp.bfloat16)
    gate_act = jax.nn.sigmoid(projected[..., 4 * tri_dim:])
    product = jnp.einsum(form, left_act.astype(jnp.float32), right_act.astype(jnp.float32))
    return gate_act * linear(layer_norm(product), w_out)


def tri_attention(pair_act, pair_mask, w_qkvg, w_bias, w_out):
    pair_norm = layer_norm(pair_act)
    pair_bias = jnp.transpose(linear(pair_norm, w_bias).astype(jnp.bfloat16), (2, 0, 1))
    return lax.map(lambda item: attend_row(item[0], pair_bias, item[1], w_qkvg, w_out, w_bias.shape[1]), (pair_norm, pair_mask))


def evoformer_block(msa_act, pair_act, msa_mask, pair_mask, layer_w):
    (row_qkvg, row_bias, row_out, col_qkvg, col_out, mtr_in, mtr_out, opm_proj, opm_out,
     tmo_proj, tmo_out, tmi_proj, tmi_out, tas_qkvg, tas_bias, tas_out,
     tae_qkvg, tae_bias, tae_out, ptr_in, ptr_out) = layer_w
    msa_act = residual(msa_act, row_attention(msa_act, pair_act, msa_mask, row_qkvg, row_bias, row_out))
    msa_act = residual(msa_act, column_attention(msa_act, msa_mask, col_qkvg, col_out, row_bias.shape[1]))
    msa_act = residual(msa_act, transition(msa_act, mtr_in, mtr_out))
    pair_act = residual(pair_act, outer_product_mean(msa_act, msa_mask, opm_proj, opm_out))
    pair_act = residual(pair_act, tri_mul(pair_act, pair_mask, tmo_proj, tmo_out, 'ikc,jkc->ijc'))
    pair_act = residual(pair_act, tri_mul(pair_act, pair_mask, tmi_proj, tmi_out, 'kic,kjc->ijc'))
    pair_act = residual(pair_act, tri_attention(pair_act, pair_mask, tas_qkvg, tas_bias, tas_out))
    pair_swap = jnp.swapaxes(pair_act, 0, 1)
    pair_act = residual(pair_act, jnp.swapaxes(tri_attention(pair_swap, pair_mask.T, tae_qkvg, tae_bias, tae_out), 0, 1))
    pair_act = residual(pair_act, transition(pair_act, ptr_in, ptr_out))
    return msa_act, pair_act


def reference(msa_act, pair_act, msa_mask, pair_mask, row_qkvg, row_bias, row_out, col_qkvg, col_out, mtr_in, mtr_out, opm_proj, opm_out, tmo_proj, tmo_out, tmi_proj, tmi_out, tas_qkvg, tas_bias, tas_out, tae_qkvg, tae_bias, tae_out, ptr_in, ptr_out):
    stacked = (row_qkvg, row_bias, row_out, col_qkvg, col_out, mtr_in, mtr_out, opm_proj, opm_out,
               tmo_proj, tmo_out, tmi_proj, tmi_out, tas_qkvg, tas_bias, tas_out,
               tae_qkvg, tae_bias, tae_out, ptr_in, ptr_out)

    def step(carry, layer_w):
        return evoformer_block(carry[0], carry[1], msa_mask, pair_mask, layer_w), None

    carried, ignored = lax.scan(step, (msa_act, pair_act), stacked)
    return carried[0], carried[1]
```

```python
import functools

import jax
import jax.numpy as jnp
from jax import lax
from jax.experimental import pallas as pl
from jax.experimental.pallas import tpu as pltpu
from jax.sharding import PartitionSpec as P

GROUP_AXIS = 'dap'
PARTS_AXIS = 'req'
LOG2E = 1.4426950408889634
MASKED = -1e9 * LOG2E
HEAD = 32
F32 = jnp.float32
BF16 = jnp.bfloat16
VMEM_LIMIT = 60 * 1024 * 1024
NT = (((1,), (1,)), ((), ()))
NN = (((1,), (0,)), ((), ()))
TN = (((0,), (0,)), ((), ()))


def dot(x, y, dims=NN):
    return lax.dot_general(x, y, dims, preferred_element_type=F32)


def layer_norm(x):
    centered = x - jnp.mean(x, axis=-1, keepdims=True)
    variance = jnp.mean(centered * centered, axis=-1, keepdims=True)
    return (centered * lax.rsqrt(variance + 1e-5)).astype(BF16)


def call(body, name, grid, in_specs, out_specs, out_shape, scratch, flops, scalars=None):
    n_scalar = 0 if scalars is None else 1
    spec = pltpu.PrefetchScalarGridSpec(num_scalar_prefetch=n_scalar, grid=grid, in_specs=in_specs, out_specs=out_specs, scratch_shapes=scratch)
    return pl.pallas_call(
        body, name=name, grid_spec=spec, out_shape=out_shape,
        compiler_params=pltpu.CompilerParams(vmem_limit_bytes=VMEM_LIMIT, dimension_semantics=('arbitrary',) * len(grid)),
        cost_estimate=pl.CostEstimate(flops=flops, bytes_accessed=16 << 20, transcendentals=0))


def head_masks(width):
    lanes = lax.broadcasted_iota(jnp.int32, (1, width), 1) // HEAD
    keep = [lanes == h for h in range(width // HEAD)]
    return keep, [k.astype(F32).astype(BF16) for k in keep]


def attend(q, k, v, bias, key_ok):
    keep, mult = head_masks(q.shape[1])
    out = jnp.zeros(q.shape, F32)
    for h in range(len(keep)):
        logits = dot(q * mult[h], k, NT) * (HEAD ** -0.5 * LOG2E)
        if bias is not None:
            logits = logits + bias(h)
        logits = jnp.where(key_ok, logits, MASKED)
        top = jnp.max(logits, axis=-1, keepdims=True)
        weights = jnp.exp2(logits - top)
        prob = (weights * (1.0 / jnp.sum(weights, axis=-1, keepdims=True))).astype(BF16)
        out = jnp.where(keep[h], dot(prob, v), out)
    return out


def gated_attention(x_norm, w_qkvg, w_out, bias, key_ok):
    width = w_out.shape[0]
    proj = dot(x_norm, w_qkvg).astype(BF16)
    parts = []
    for g in range(width // 128):
        q, k, v, gate = (proj[:, p * width + g * 128:p * width + (g + 1) * 128] for p in range(4))
        attended = attend(q, k, v, None if bias is None else functools.partial(bias, g), key_ok)
        parts.append((attended * jax.nn.sigmoid(gate.astype(F32))).astype(BF16))
    gated = parts[0] if len(parts) == 1 else jnp.concatenate(parts, axis=1)
    return dot(gated, w_out)


def put_row(scr, r, value, step):
    for p in range(scr.shape[0]):
        scr[p, pl.ds(r, value.shape[0], stride=step), :] = value[:, p * 128:(p + 1) * 128]


def flush_rows(scr, out_ref, step):
    n = scr.shape[1] // step
    for p in range(scr.shape[0]):
        out_ref[:, :, p * 128:(p + 1) * 128] = scr[p].reshape(n, step, 128)[:out_ref.shape[0]].astype(BF16)


def whole(shape):
    return pl.BlockSpec(shape, lambda *_: (0,) * len(shape))


def layer_w(w, layer):
    return pl.BlockSpec((None,) + w.shape[1:], lambda *_: (layer, 0, 0))


def row_bias(z, w_t, layer):
    rows, cols, dim = z.shape
    heads = w_t.shape[1]
    step = 16

    def body(z_ref, w_ref, out_ref, scr):
        def one(r, carry):
            x = layer_norm(z_ref[r].astype(F32))
            put_row(scr, r, dot(w_ref[...], x, NT), step)
            return carry
        lax.fori_loop(0, step, one, 0)
        flush_rows(scr, out_ref, step)

    return call(body, 'row_bias', (rows // step,),
                [pl.BlockSpec((step, cols, dim), lambda i: (i, 0, 0)), layer_w(w_t, layer)],
                pl.BlockSpec((heads, step, cols), lambda i: (0, i, 0)),
                jax.ShapeDtypeStruct((heads, rows, cols), BF16),
                [pltpu.VMEM((cols // 128, heads * step, 128), F32)], 10 ** 9)(z, w_t)


def fill_bias(bias_ref, scr, swap):
    blocks, heads, rows, cols = bias_ref.shape
    for h in range(heads):
        full = jnp.concatenate([bias_ref[b, h].astype(F32) for b in range(blocks)], axis=0) * LOG2E
        scr[h] = full.T if swap else full


def row_attention(m, bias, mask, w_qkvg, w_out, layer, swap):
    n_seq, res, dim = m.shape
    heads = bias.shape[1]

    def body(m_ref, bias_ref, mask_ref, wq_ref, wo_ref, out_ref, scr):
        @pl.when(pl.program_id(0) == 0)
        def _():
            fill_bias(bias_ref, scr, swap)
        x = m_ref[0].astype(F32)
        update = gated_attention(layer_norm(x), wq_ref[...], wo_ref[...], lambda g, h: scr[g * 4 + h], mask_ref[0] > 0)
        out_ref[0] = (x + update).astype(BF16)

    return call(body, 'row_attention', (n_seq,),
                [pl.BlockSpec((1, res, dim), lambda s: (s, 0, 0)), whole(bias.shape),
                 pl.BlockSpec((1, 1, res), lambda s: (s, 0, 0)), layer_w(w_qkvg, layer), layer_w(w_out, layer)],
                pl.BlockSpec((1, res, dim), lambda s: (s, 0, 0)), jax.ShapeDtypeStruct(m.shape, BF16),
                [pltpu.VMEM((heads, res, res), F32)], 4 * 10 ** 10)(m, bias, mask, w_qkvg, w_out)


def column_stage(m, mask_t, w_qkvg, w_out, w_in, w_down, w_opm_t, layer):
    n_seq, res, dim = m.shape
    step = 16
    opm = w_opm_t.shape[1]

    def body(m_ref, mask_ref, wq_ref, wo_ref, wi_ref, wd_ref, wp_ref, out_ref, ab_ref, lo, hi, x_scr, att):
        halves = (lo, hi)
        for p in range(2):
            halves[p][...] = m_ref[:, :, p * 128:(p + 1) * 128].astype(F32).reshape(n_seq * step, 128)

        def gather(r, carry):
            at = pl.ds(pl.multiple_of(r * n_seq, n_seq), n_seq)
            for p in range(2):
                x_scr[at, p * 128:(p + 1) * 128] = halves[p][pl.ds(r, n_seq, stride=step), :]
            return carry
        lax.fori_loop(0, step, gather, 0)

        def one(r, carry):
            at = pl.ds(pl.multiple_of(r * n_seq, n_seq), n_seq)
            proj = dot(layer_norm(x_scr[at, :]), wq_ref[...]).astype(BF16)
            key_ok = mask_ref[r] > 0
            keep, mult = head_masks(128)
            for g in range(2):
                q, k, v, gate = (proj[:, p * 256 + g * 128:p * 256 + (g + 1) * 128] for p in range(4))
                stacked = jnp.concatenate([q * mult[h] for h in range(4)], axis=0)
                logits = dot(stacked, k, NT) * (HEAD ** -0.5 * LOG2E)
                logits = jnp.where(key_ok, logits, MASKED)
                weights = jnp.exp2(logits - jnp.max(logits, axis=-1, keepdims=True))
                prob = (weights * (1.0 / jnp.sum(weights, axis=-1, keepdims=True))).astype(BF16)
                full = dot(prob, v)
                attended = jnp.zeros((n_seq, 128), F32)
                for h in range(4):
                    attended = jnp.where(keep[h], full[h * n_seq:(h + 1) * n_seq], attended)
                att[at, g * 128:(g + 1) * 128] = (attended * jax.nn.sigmoid(gate.astype(F32))).astype(BF16)
            return carry
        lax.fori_loop(0, step, one, 0)

        x = x_scr[...] + dot(att[...], wo_ref[...])
        x = x.astype(BF16).astype(F32)
        hidden = jnp.maximum(dot(layer_norm(x), wi_ref[...]), 0.0).astype(BF16)
        x = (x + dot(hidden, wd_ref[...])).astype(BF16).astype(F32)
        x_scr[...] = x

        def project(r, carry):
            at = pl.ds(pl.multiple_of(r * n_seq, n_seq), n_seq)
            x_r = x_scr[at, :]
            ab = dot(wp_ref[...], layer_norm(x_r), NT).astype(BF16)
            ab_ref[r] = (ab.astype(F32) * mask_ref[r].astype(F32)).astype(BF16)
            for p in range(2):
                halves[p][pl.ds(r, n_seq, stride=step), :] = x_r[:, p * 128:(p + 1) * 128]
            return carry
        lax.fori_loop(0, step, project, 0)
        for p in range(2):
            out_ref[:, :, p * 128:(p + 1) * 128] = halves[p][...].reshape(n_seq, step, 128).astype(BF16)

    return call(body, 'column_stage', (res // step,),
                [pl.BlockSpec((n_seq, step, dim), lambda i: (0, i, 0)), pl.BlockSpec((step, 1, n_seq), lambda i: (i, 0, 0))]
                + [layer_w(w, layer) for w in (w_qkvg, w_out, w_in, w_down, w_opm_t)],
                (pl.BlockSpec((n_seq, step, dim), lambda i: (0, i, 0)), pl.BlockSpec((step, opm, n_seq), lambda i: (i, 0, 0))),
                (jax.ShapeDtypeStruct(m.shape, BF16), jax.ShapeDtypeStruct((res, opm, n_seq), BF16)),
                [pltpu.VMEM((n_seq * step, 128), F32), pltpu.VMEM((n_seq * step, 128), F32),
                 pltpu.VMEM((n_seq * step, dim), F32), pltpu.VMEM((n_seq * step, dim), BF16)],
                4 * 10 ** 10)(m, mask_t, w_qkvg, w_out, w_in, w_down, w_opm_t)


def outer_product(z, left, right, mask_left, mask_right, w_opm, where, layer, by_cols):
    opm = w_opm.shape[2] // 32
    res = right.shape[1]
    n_seq = right.shape[2]
    step = 8
    half = res // 2

    def body(where_ref, z_ref, left_ref, right_ref, ml_ref, mr_ref, w_ref, out_ref, pairs):
        lhs = left_ref[...].reshape(step * opm, n_seq)

        def outer(e, carry):
            full = dot(lhs, right_ref[e], NT).astype(BF16)
            at = pl.ds(pl.multiple_of(e * opm, opm), opm)
            for r in range(step):
                pairs[r, at, :] = full[r * opm:(r + 1) * opm]
            return carry
        lax.fori_loop(0, opm, outer, 0, unroll=4)
        overlap = dot(ml_ref[...], mr_ref[...])
        scale = 1.0 / (1e-3 + overlap)
        for r in range(step):
            update = dot(w_ref[...], pairs[r]) * scale[r:r + 1]
            if by_cols:
                old = jnp.concatenate([z_ref[b, r] for b in range(z_ref.shape[0])], axis=0)
            else:
                old = z_ref[0, r]
            out_ref[r] = (old.astype(F32) + update.T).astype(BF16)

    blocks = z.shape[0]
    per_block = res // blocks // step
    if by_cols:
        z_spec = pl.BlockSpec((blocks, step, z.shape[2], z.shape[3]), lambda t, s: (0, ((t // per_block) * 2 + s[0]) * per_block + t % per_block, 0, 0))
    else:
        z_spec = pl.BlockSpec((1, step, z.shape[2], z.shape[3]), lambda t, s: ((t // per_block) * 2 + s[0], t % per_block, 0, 0))
    row_of = lambda t, s: ((t // per_block) * 2 + s[0]) * per_block + t % per_block
    return call(body, 'outer_product', (half // step,),
                [z_spec, pl.BlockSpec((step, opm, n_seq), lambda t, s: (row_of(t, s), 0, 0)), whole(right.shape),
                 pl.BlockSpec((step, n_seq), lambda t, s: (row_of(t, s), 0)), whole(mask_right.shape), layer_w(w_opm, layer)],
                pl.BlockSpec((step, res, z.shape[3]), lambda t, s: (t, 0, 0)),
                jax.ShapeDtypeStruct((half, res, z.shape[3]), BF16),
                [pltpu.VMEM((step, opm * opm, res), BF16)], 2 * 10 ** 10, where)(where, z, left, right, mask_left, mask_right, w_opm)


def triangle_project(z, mask, w_t, where, layer, chip_cols):
    rows, cols, dim = z.shape
    tri = (w_t.shape[1] - dim) // 4
    step = 16
    a_cols = cols // 2 if chip_cols else cols

    def body(where_ref, z_ref, mask_ref, w_ref, a_ref, b_ref, a_scr, b_scr):
        def one(r, carry):
            x = layer_norm(z_ref[r].astype(F32))
            proj = dot(w_ref[:4 * tri, :], x, NT)
            mask_row = mask_ref[r]
            a, b, ga, gb = (proj[p * tri:(p + 1) * tri] for p in range(4))
            mask_a = mask_row
            if chip_cols:
                first = where_ref[1] == 0
                a, ga, mask_a = (jnp.where(first, v[:, :a_cols], v[:, a_cols:]) for v in (a, ga, mask_row))
            a = mask_a * jax.nn.sigmoid(ga) * a
            b = mask_row * jax.nn.sigmoid(gb) * b
            put_row(a_scr, r, a, step)
            put_row(b_scr, r, b, step)
            return carry
        lax.fori_loop(0, step, one, 0)
        flush_rows(a_scr, a_ref, step)
        flush_rows(b_scr, b_ref, step)

    return call(body, 'triangle_project', (rows // step,),
                [pl.BlockSpec((step, cols, dim), lambda i, s: (i, 0, 0)), pl.BlockSpec((step, 1, cols), lambda i, s: (i, 0, 0)), layer_w(w_t, layer)],
                (pl.BlockSpec((tri, step, a_cols), lambda i, s: (0, i, 0)), pl.BlockSpec((tri, step, cols), lambda i, s: (0, i, 0))),
                (jax.ShapeDtypeStruct((tri, rows, a_cols), BF16), jax.ShapeDtypeStruct((tri, rows, cols), BF16)),
                [pltpu.VMEM((a_cols // 128, tri * step, 128), F32), pltpu.VMEM((cols // 128, tri * step, 128), F32)],
                2 * 10 ** 10, where)(where, z, mask, w_t)


def triangle_finish(z, a, b, w_proj, w_out, where, layer, incoming, w_bias_t=None):
    half, res, dim = z.shape
    tri = b.shape[1]
    quarter = half // 2
    rows_out = quarter if incoming else half
    ch = 8
    step = 16
    n_prod = tri // ch
    n_fin = rows_out // step
    heads = 0 if w_bias_t is None else w_bias_t.shape[1]
    pad = 8

    def body(where_ref, z_ref, a_ref, b_ref, wp_ref, wo_ref, *rest):
        if heads:
            wb_ref, out_ref, bias_ref, prod, norm, bias_scr = rest
        else:
            out_ref, prod, norm = rest
        t = pl.program_id(0)

        @pl.when(t < n_prod)
        def _():
            for c in range(ch):
                if incoming:
                    x = dot(a_ref[0, c], b_ref[0, c], TN) + dot(a_ref[1, c], b_ref[1, c], TN)
                else:
                    rhs = jnp.concatenate([b_ref[0, c, :quarter], b_ref[1, c, :quarter], b_ref[0, c, quarter:], b_ref[1, c, quarter:]], axis=0)
                    x = dot(a_ref[c], rhs, NT)
                prod[t * ch + c] = x

        @pl.when(t >= n_prod)
        def _():
            first = (t - n_prod) * step
            if incoming:
                first = first + where_ref[0] * quarter
            x = prod[:, pl.ds(pl.multiple_of(first, step), step), :]
            centered = x - jnp.mean(x, axis=0, keepdims=True)
            variance = jnp.mean(centered * centered, axis=0, keepdims=True)
            normed = centered * lax.rsqrt(variance + 1e-5)
            for p in range(res // 128):
                norm[p] = normed[:, :, p * 128:(p + 1) * 128].reshape(tri * step, 128)

            def one(r, carry):
                z_r = z_ref[r].astype(F32)
                gate = jax.nn.sigmoid(dot(layer_norm(z_r), wp_ref[:, 4 * tri:]))
                update = jnp.concatenate([dot(norm[p, pl.ds(r, tri, stride=step), :].astype(BF16), wo_ref[...], TN) for p in range(res // 128)], axis=0)
                new = (z_r + gate * update).astype(BF16)
                out_ref[r] = new
                if heads:
                    put_row(bias_scr, r, dot(wb_ref[...], layer_norm(new.astype(F32)), NT), step)
                return carry
            lax.fori_loop(0, step, one, 0)
            if heads:
                flush_rows(bias_scr, bias_ref, step)

    fin = lambda t: jnp.maximum(t - n_prod, 0)
    first_row = (lambda s: s[1] * (quarter // step)) if incoming else (lambda s: 0)
    prod_at = lambda t: jnp.minimum(t, n_prod - 1)
    if incoming:
        a_spec = pl.BlockSpec((2, ch) + a.shape[2:], lambda t, s: (0, prod_at(t), 0, 0))
    else:
        a_spec = pl.BlockSpec((ch,) + a.shape[1:], lambda t, s: (prod_at(t), 0, 0))
    n_heads = heads and 4
    in_specs = [pl.BlockSpec((step, res, dim), lambda t, s: (first_row(s) + fin(t), 0, 0)), a_spec,
                pl.BlockSpec((2, ch) + b.shape[2:], lambda t, s: (0, prod_at(t), 0, 0)), layer_w(w_proj, layer), layer_w(w_out, layer)]
    out_specs = [pl.BlockSpec((step, res, dim), lambda t, s: (fin(t), 0, 0))]
    out_shape = [jax.ShapeDtypeStruct((rows_out, res, dim), BF16)]
    rows_prod = a.shape[-1] if incoming else half
    scratch = [pltpu.VMEM((tri, rows_prod, res), F32), pltpu.VMEM((res // 128, tri * step, 128), F32)]
    args = [where, z, a, b, w_proj, w_out]
    if heads:
        in_specs.append(layer_w(w_bias_t, layer))
        out_specs.append(pl.BlockSpec((n_heads, step, res), lambda t, s: (0, fin(t), 0)))
        out_shape.append(jax.ShapeDtypeStruct((n_heads, rows_out, res), BF16))
        scratch.append(pltpu.VMEM((res // 128, pad * step, 128), F32))
        args.append(w_bias_t)
    return call(body, 'triangle_in' if incoming else 'triangle_out', (n_prod + n_fin,), in_specs, tuple(out_specs), tuple(out_shape), scratch, 2 * 10 ** 10, where)(*args)


def start_attention(z, bias, mask, w_qkvg, w_out, w_bias_t, layer):
    rows, res, dim = z.shape
    heads = bias.shape[1]
    step = 16
    pad = w_bias_t.shape[1]

    def body(z_ref, bias_ref, mask_ref, wq_ref, wo_ref, wb_ref, out_ref, next_ref, scr, bias_scr):
        @pl.when(pl.program_id(0) == 0)
        def _():
            fill_bias(bias_ref, scr, False)

        def one(r, carry):
            x = z_ref[r].astype(F32)
            update = gated_attention(layer_norm(x), wq_ref[...], wo_ref[...], lambda g, h: scr[h], mask_ref[r] > 0)
            new = (x + update).astype(BF16)
            out_ref[r] = new
            put_row(bias_scr, r, dot(wb_ref[...], layer_norm(new.astype(F32)), NT), step)
            return carry
        lax.fori_loop(0, step, one, 0)
        flush_rows(bias_scr, next_ref, step)

    return call(body, 'start_attention', (rows // step,),
                [pl.BlockSpec((step, res, dim), lambda i: (i, 0, 0)), whole(bias.shape), pl.BlockSpec((step, 1, res), lambda i: (i, 0, 0)),
                 layer_w(w_qkvg, layer), layer_w(w_out, layer), layer_w(w_bias_t, layer)],
                (pl.BlockSpec((step, res, dim), lambda i: (i, 0, 0)), pl.BlockSpec((heads, step, res), lambda i: (0, i, 0))),
                (jax.ShapeDtypeStruct(z.shape, BF16), jax.ShapeDtypeStruct((heads, rows, res), BF16)),
                [pltpu.VMEM((heads, res, res), F32), pltpu.VMEM((res // 128, pad * step, 128), F32)],
                5 * 10 ** 10)(z, bias, mask, w_qkvg, w_out, w_bias_t)


def end_stage(z, bias, mask_t, w_qkvg, w_out, w_in, w_down, w_bias_t, layer, next_layer):
    res, cols, dim = z.shape
    heads = bias.shape[1]
    step = 16
    pad = w_bias_t.shape[1]

    def body(z_ref, bias_ref, mask_ref, wq_ref, wo_ref, wi_ref, wd_ref, wb_ref, out_ref, next_ref, scr, rows, bias_scr):
        @pl.when(pl.program_id(0) == 0)
        def _():
            fill_bias(bias_ref, scr, True)
        rows[...] = z_ref[...].astype(F32).reshape(res * step, dim)

        def one(r, carry):
            at = pl.ds(r, res, stride=step)
            x = rows[at, :]
            x = x + gated_attention(layer_norm(x), wq_ref[...], wo_ref[...], lambda g, h: scr[h], mask_ref[r] > 0)
            x = x.astype(BF16).astype(F32)
            hidden = jnp.maximum(dot(layer_norm(x), wi_ref[...]), 0.0).astype(BF16)
            x = (x + dot(hidden, wd_ref[...])).astype(BF16).astype(F32)
            rows[at, :] = x
            put_row(bias_scr, r, dot(wb_ref[...], layer_norm(x), NT), step)
            return carry
        lax.fori_loop(0, step, one, 0)
        out_ref[...] = rows[...].reshape(res, step, dim).astype(BF16)
        flush_rows(bias_scr, next_ref, step)

    return call(body, 'end_stage', (cols // step,),
                [pl.BlockSpec((res, step, dim), lambda i: (0, i, 0)), whole(bias.shape), pl.BlockSpec((step, 1, res), lambda i: (i, 0, 0))]
                + [layer_w(w, layer) for w in (w_qkvg, w_out, w_in, w_down)] + [layer_w(w_bias_t, next_layer)],
                (pl.BlockSpec((res, step, dim), lambda i: (0, i, 0)), pl.BlockSpec((pad, step, res), lambda i: (0, i, 0))),
                (jax.ShapeDtypeStruct(z.shape, BF16), jax.ShapeDtypeStruct((pad, cols, res), BF16)),
                [pltpu.VMEM((heads, res, res), F32), pltpu.VMEM((res * step, dim), F32), pltpu.VMEM((res // 128, pad * step, 128), F32)],
                6 * 10 ** 10)(z, bias, mask_t, w_qkvg, w_out, w_in, w_down, w_bias_t)


def gather(x):
    return lax.all_gather(x, GROUP_AXIS, axis=0)


def pair_gather(x):
    return lax.all_gather(x, GROUP_AXIS, axis=0, axis_index_groups=[[0, 1], [2, 3]])


def transpose_w(w, pad=0):
    w = jnp.swapaxes(w, 1, 2)
    return jnp.pad(w, ((0, 0), (0, pad), (0, 0))) if pad else w


def solution(mesh):
    row_spec = P((PARTS_AXIS, GROUP_AXIS))

    def local_body(m, z, msa_mask, pair_mask, *weights):
        (row_qkvg, row_bias_w, row_out, col_qkvg, col_out, mtr_in, mtr_out, opm_proj, opm_out,
         tmo_proj, tmo_out, tmi_proj, tmi_out, tas_qkvg, tas_bias, tas_out,
         tae_qkvg, tae_bias, tae_out, ptr_in, ptr_out) = weights
        layers = row_qkvg.shape[0]
        shard = lax.axis_index(GROUP_AXIS)
        chip, core = shard // 2, shard % 2
        where = jnp.stack([core, chip]).astype(jnp.int32)
        n_seq, res_loc = m.shape[0], z.shape[0]
        res = z.shape[1]
        z_all = gather(z)
        full_mask = lax.all_gather(msa_mask, GROUP_AXIS, axis=0, tiled=True)
        full_pair = lax.all_gather(pair_mask, GROUP_AXIS, axis=0)
        seq_mask = msa_mask[:, None, :]
        res_mask_t = lax.dynamic_slice_in_dim(full_mask, shard * res_loc, res_loc, 1).T[:, None, :]
        mask_bf = full_mask.astype(BF16)
        mask_bf_t = mask_bf.T
        half_mask = lax.dynamic_index_in_dim(full_pair.reshape(2, 2, res_loc, res), core, 1, False)
        half_mask = half_mask.reshape(2 * res_loc, 1, res).astype(F32)
        row_mask = pair_mask[:, None, :]
        col_mask = lax.dynamic_slice_in_dim(full_pair.reshape(res, res), shard * res_loc, res_loc, 1).T[:, None, :]
        row_bias_t = transpose_w(row_bias_w)
        tas_bias_t, tae_bias_t = transpose_w(tas_bias, 4), transpose_w(tae_bias, 4)
        tmo_t, tmi_t, opm_proj_t = transpose_w(tmo_proj), transpose_w(tmi_proj), transpose_w(opm_proj)
        opm = opm_proj.shape[2] // 2
        opm_t = opm_out.reshape(layers, opm, opm, -1).transpose(0, 3, 2, 1).reshape(layers, -1, opm * opm)

        bias = row_bias(z, row_bias_t, 0)
        for layer in range(layers):
            by_cols = layer > 0
            if by_cols:
                z_all = gather(z)
            m = row_attention(m, gather(bias), seq_mask, row_qkvg, row_out, layer, by_cols)
            m = lax.all_to_all(m, GROUP_AXIS, 1, 0, tiled=True)
            m, ab = column_stage(m, res_mask_t, col_qkvg, col_out, mtr_in, mtr_out, opm_proj_t, layer)
            ab = gather(ab).reshape(res, 2 * opm, -1)
            right = jnp.swapaxes(ab[:, opm:], 0, 1)
            m = lax.all_to_all(m, GROUP_AXIS, 0, 1, tiled=True)
            half = outer_product(z_all, ab, right, mask_bf_t, mask_bf, opm_t, where, layer, by_cols)
            a, b = triangle_project(half, half_mask, tmo_t, where, layer, False)
            half, = triangle_finish(half, a, pair_gather(b), tmo_proj, tmo_out, where, layer, False)
            a, b = triangle_project(half, half_mask, tmi_t, where, layer, True)
            z, bias = triangle_finish(half, pair_gather(a), pair_gather(b), tmi_proj, tmi_out, where, layer, True, tas_bias_t)
            z, bias = start_attention(z, gather(bias), row_mask, tas_qkvg, tas_out, tae_bias_t, layer)
            bias = gather(bias)
            z = lax.all_to_all(z, GROUP_AXIS, 1, 0, tiled=True)
            z, bias = end_stage(z, bias, col_mask, tae_qkvg, tae_out, ptr_in, ptr_out, row_bias_t, layer, min(layer + 1, layers - 1))
        return m, lax.all_to_all(z, GROUP_AXIS, 0, 1, tiled=True)

    def run_blocks(*arrays):
        n_weights = len(arrays) - 4
        return jax.shard_map(local_body, mesh=mesh, in_specs=(row_spec,) * 4 + (P(),) * n_weights, out_specs=(row_spec, row_spec), check_vma=False)(*arrays)

    return run_blocks
```
